768 devices in a mesh: freq: 48 (over y_lo, z), cell: 16 (over x, y_hi, core).
Axes of the slice: x: 4, y: 8 (y_hi: 2, y_lo: 4; y = y_hi * 4 + y_lo), z: 12, core: 2. Of those that a mesh axis runs over, the one named last changes fastest.
Arguments:
- columns: float32 [2, 96, 384, 600], P(None, 'freq'), may hold values from -6 to 6
- freq_blocks: float32 [2, 96, 600, 4096], P(None, 'freq', None, 'cell'), may hold values from -0.09375 to 0.09375
- causal_cutoffs: int32 [384], replicated, may hold values from 23 to 95
- band_index: int32 [4096], P('cell'), may hold values from 0 to 7
- band_rates: float32 [8], replicated, may hold values from 0.05 to 0.45
Outputs:
- hessian_columns: float32 [2, 96, 384, 600], P(None, 'freq', 'cell')
The draws below stay inside these ranges and needn't reach their ends.
All inputs are finite; a program needn't handle non-finite values.
Results may differ from the reference program's by a relative error of at most 0.00007.
Values sent between devices are 32-bit elements; how exact they have to be, the bound alone decides.
A program may use at most 64 MiB of HBM per device.

```python
import math
import jax
import jax.numpy as jnp
from jax import lax

NS = 600
SWEEPS = 4
BANDS = 8
NF = 96
EPOCH_LENGTH = 95
CURVATURE_RANKS = 384
NM = 4096


def place_ends(result, stream_key, least, largest):
    longest = result.shape.index(max(result.shape))
    spots = []
    for shift in (0, 1):
        where = [jax.random.randint(jax.random.fold_in(stream_key, axis), (), 0, length) for axis, length in enumerate(result.shape)]
        where[longest] = (where[longest] + shift) % result.shape[longest]
        spots.append(tuple(where))
    return result.at[spots[0]].set(least).at[spots[1]].set(largest)


def level_of(key, shape, split, smallest, top_value):
    level, own = 1.0, jax.random.fold_in(key, 6)
    for dim, shards_of in split:
        steps = jnp.exp(jax.random.uniform(jax.random.fold_in(own, dim), (shards_of,), jnp.float32, smallest / len(split), top_value / len(split)))
        level = level * jnp.repeat(steps, shape[dim] // shards_of).reshape([-1 if axis == dim else 1 for axis in range(len(shape))])
    return level


def scatter_about(rng, shape, width, most, cuts=(), dtype=jnp.bfloat16):
    drawn = width * jax.random.normal(rng, shape, jnp.float32)
    if cuts:
        drawn = drawn * level_of(rng, shape, cuts, -0.22, 0.18)
    return jnp.clip(drawn, -most, most).astype(dtype)


def setup_inputs(seed: int = 0) -> dict:
    streams_of = jax.random.split(jax.random.key(seed), 6)
    columns = scatter_about(streams_of[0], (2, NF, CURVATURE_RANKS, NS), 1.0, 6.0, ((1, 48),), jnp.float32)
    freq_blocks = scatter_about(streams_of[1], (2, NF, NS, NM), NM ** -0.5, 0.09375, ((1, 48), (3, 16)), jnp.float32)
    causal_cutoffs = place_ends(jax.random.randint(streams_of[2], (CURVATURE_RANKS,), EPOCH_LENGTH // 4, EPOCH_LENGTH + 1), jax.random.fold_in(streams_of[2], 1), EPOCH_LENGTH // 4, EPOCH_LENGTH).astype(jnp.int32)
    band_index = place_ends(jax.random.randint(streams_of[3], (NM,), 0, BANDS), jax.random.fold_in(streams_of[3], 1), 0, BANDS - 1).astype(jnp.int32)
    band_rates = jnp.clip(jax.random.uniform(streams_of[4], (BANDS,), jnp.float32, 0.05, 0.45), 0.05, 0.45)
    return {"columns": columns, "freq_blocks": freq_blocks, "causal_cutoffs": causal_cutoffs, "band_index": band_index, "band_rates": band_rates}


precise = lax.Precision.HIGHEST


def inverse_table(epoch_number, harmonic_number):
    cycle_length = 2 * epoch_number
    sample_moments = lax.broadcasted_iota(jnp.int32, (epoch_number, harmonic_number), 0)
    harmonic_rate = lax.broadcasted_iota(jnp.int32, (epoch_number, harmonic_number), 1)
    harmonic_offsets = ((sample_moments * harmonic_rate) % cycle_length).astype(jnp.float32) * (2.0 * math.pi / cycle_length)
    weight = jnp.where((harmonic_rate == 0) | (harmonic_rate == harmonic_number - 1), 1.0, 2.0).astype(jnp.float32) / cycle_length
    return jnp.concatenate([weight * jnp.cos(harmonic_offsets), -weight * jnp.sin(harmonic_offsets)], axis=1)


def forward_table(epoch_number, harmonic_number):
    cycle_length = 2 * epoch_number
    harmonic_rate = lax.broadcasted_iota(jnp.int32, (harmonic_number, epoch_number), 0)
    sample_moments = lax.broadcasted_iota(jnp.int32, (harmonic_number, epoch_number), 1)
    harmonic_offsets = ((sample_moments * harmonic_rate) % cycle_length).astype(jnp.float32) * (2.0 * math.pi / cycle_length)
    return jnp.concatenate([jnp.cos(harmonic_offsets), -jnp.sin(harmonic_offsets)], axis=0)


def adjoint_product(columns, blocks):
    real_part = jnp.einsum('kjs,ksm->kjm', columns[0], blocks[0], precision=precise) + jnp.einsum('kjs,ksm->kjm', columns[1], blocks[1], precision=precise)
    imag_part = jnp.einsum('kjs,ksm->kjm', columns[1], blocks[0], precision=precise) - jnp.einsum('kjs,ksm->kjm', columns[0], blocks[1], precision=precise)
    return jnp.stack([real_part, imag_part])


def forward_product(spectrum, blocks):
    real_part = jnp.einsum('kjm,ksm->kjs', spectrum[0], blocks[0], precision=precise) - jnp.einsum('kjm,ksm->kjs', spectrum[1], blocks[1], precision=precise)
    imag_part = jnp.einsum('kjm,ksm->kjs', spectrum[1], blocks[0], precision=precise) + jnp.einsum('kjm,ksm->kjs', spectrum[0], blocks[1], precision=precise)
    return jnp.stack([real_part, imag_part])


def reference(columns, freq_blocks, causal_cutoffs, band_index, band_rates):
    spectrum = adjoint_product(columns, freq_blocks)
    sampled_trace = jnp.dot(inverse_table(EPOCH_LENGTH, NF), spectrum.reshape(2 * NF, CURVATURE_RANKS * NM), precision=precise, preferred_element_type=jnp.float32)
    sampled_trace = sampled_trace.reshape(EPOCH_LENGTH, CURVATURE_RANKS, NM)
    sample_moments = lax.broadcasted_iota(jnp.int32, (EPOCH_LENGTH, CURVATURE_RANKS), 0)
    sampled_trace = jnp.where((sample_moments < causal_cutoffs[None, :])[:, :, None], sampled_trace, 0.0)
    cell_rates = jnp.take(band_rates, band_index)
    for repeat in range(SWEEPS):
        padded = jnp.pad(sampled_trace, ((0, 0), (0, 0), (1, 1)))
        sampled_trace = sampled_trace + cell_rates * (padded[:, :, :-2] - 2.0 * sampled_trace + padded[:, :, 2:])
    spectrum = jnp.dot(forward_table(EPOCH_LENGTH, NF), sampled_trace.reshape(EPOCH_LENGTH, CURVATURE_RANKS * NM), precision=precise, preferred_element_type=jnp.float32)
    spectrum = spectrum.reshape(2, NF, CURVATURE_RANKS, NM)
    return forward_product(spectrum, freq_blocks)
```

```python
import math

import jax
import jax.numpy as jnp
import numpy as np
from jax import lax
from jax.experimental import pallas as pl
from jax.experimental.pallas import tpu as pltpu
from jax.sharding import Mesh
from jax.sharding import PartitionSpec as P

AXES = ("ylo", "z", "x", "yhi", "core")
YLO, ZED, EX, YHI, CORES = 4, 12, 4, 2, 2
FREQ_DEVICES = YLO * ZED
NF = 96
NT = 95
TP = 96
NS = 600
NSP = 640
NJ = 384
JD = 8
CD = 256
SWEEPS = 4
BANDS = 8
OUT_COLS = 24
MESH = pl.DeviceIdType.MESH
F32, BF16 = jnp.float32, jnp.bfloat16


def halves(table):
    high = table.astype(np.float32).astype(jnp.bfloat16)
    low = (table - high.astype(np.float64)).astype(jnp.bfloat16)
    return high, low


def tables():
    cycle = 2 * NT
    k = np.arange(NF)
    t = np.arange(NT)
    angle = 2.0 * math.pi * ((t[:, None] * k[None, :]) % cycle) / cycle
    weight = np.where((k == 0) | (k == NF - 1), 1.0, 2.0) / cycle
    inv = np.stack([weight * np.cos(angle), -weight * np.sin(angle)], axis=-1)
    inv = inv.reshape(NT, FREQ_DEVICES, 2, 2).transpose(0, 2, 1, 3).reshape(NT, 2 * NF)
    inv = np.concatenate([inv, np.zeros((TP - NT, 2 * NF))], axis=0)
    fwd = np.stack([np.cos(angle), -np.sin(angle)], axis=-1)
    fwd = fwd.reshape(NT, FREQ_DEVICES, 2, 2).transpose(2, 1, 3, 0).reshape(2, NF, NT)
    fwd = np.concatenate([fwd, np.zeros((2, NF, TP - NT))], axis=2)
    return (
        np.concatenate(halves(inv), axis=0),
        np.concatenate(halves(fwd), axis=1),
    )


def split(x):
    high = x.astype(BF16)
    return high, (x - high.astype(F32)).astype(BF16)


def mm(a, b):
    return lax.dot_general(a, b, (((1,), (0,)), ((), ())), preferred_element_type=F32)


def mt(a, b):
    return lax.dot_general(a, b, (((1,), (1,)), ((), ())), preferred_element_type=F32)


def kernel(
    cut_ref, rates_ref, cols_ref, blocks_ref, bands_ref, inv_ref, fwd_ref, out_ref,
    cols, blocks, vh, vl, gh, gl, adj, got1, ext, uh, ul, rate, pack, halo, send2, got2,
    part, r1, r2a, r2b, r3,
    load_sem, self_sem, send_sem1, recv_sem1, send_sem2, recv_sem2, hsend, hrecv, rsend, rrecv,
):
    y, z = lax.axis_index("ylo"), lax.axis_index("z")
    x, yhi, core = lax.axis_index("x"), lax.axis_index("yhi"), lax.axis_index("core")
    me = y * ZED + z
    cell = (x * YHI + yhi) * CORES + core
    swap = x + 1 - 2 * lax.rem(x, 2)
    flip = 3 - x
    flip_swap = flip + 1 - 2 * lax.rem(flip, 2)

    loads = []
    for k in range(2):
        loads.append(pltpu.make_async_copy(blocks_ref.at[:, k], blocks.at[k], load_sem.at[2 * k]))
        loads.append(pltpu.make_async_copy(cols_ref.at[:, k], cols.at[k], load_sem.at[2 * k + 1]))
    for copy in loads:
        copy.start()

    def peer(i):
        turn = lax.rem(i, 4)
        step = lax.div(i, 4)
        half = 5 - lax.div(step - 1, 2)
        up = lax.rem(step, 2) == 1
        dz = jnp.where(step == 0, 6, jnp.where(up, half, 12 - half))
        dz = jnp.where(step == 11, 0, dz)
        return lax.rem(y + 3 - turn, YLO), lax.rem(z + dz, ZED)

    def cell_peer(c):
        c = lax.rem(c + 16, 16)
        return {"x": lax.div(c, 4), "yhi": lax.rem(lax.div(c, 2), 2), "core": lax.rem(c, 2)}

    left, right = cell_peer(cell - 1), cell_peer(cell + 1)
    sibling, over = {"core": 1 - core}, {"yhi": 1 - yhi}

    barrier = pltpu.get_barrier_semaphore()

    def greet(i, carry):
        py, pz = peer(i)
        pl.semaphore_signal(barrier, inc=1, device_id={"ylo": py, "z": pz}, device_id_type=MESH)
        return carry

    lax.fori_loop(0, FREQ_DEVICES - 1, greet, 0)
    friends = [left, right, sibling, over, {"x": swap}, {"x": flip}]
    for friend in friends:
        pl.semaphore_signal(barrier, inc=1, device_id=friend, device_id_type=MESH)

    vh[...] = jnp.zeros_like(vh)
    vl[...] = jnp.zeros_like(vl)

    def operands(k):
        blank = jnp.zeros((NSP - NS, CD), F32)
        for part_index in range(2):
            value = jnp.concatenate([blocks[k, part_index], blank], axis=0)
            high, low = split(value)
            for into, half in ((gh, high), (gl, low)):
                if part_index == 0:
                    into[k, 0:NSP, 0:CD] = half
                    into[k, NSP:, CD:] = half
                else:
                    into[k, 0:NSP, CD:] = -half
                    into[k, NSP:, 0:CD] = half
            high, low = split(cols[k, part_index])
            vh[:, part_index * NSP : part_index * NSP + NS] = high
            vl[:, part_index * NSP : part_index * NSP + NS] = low

    def exchange(k, source, target, send_sem, recv_sem):
        def send(i, carry):
            py, pz = peer(i)
            dest = py * ZED + pz
            pltpu.make_async_remote_copy(
                src_ref=source(k, dest),
                dst_ref=target(k, me),
                send_sem=send_sem.at[k],
                recv_sem=recv_sem.at[k],
                device_id={"ylo": py, "z": pz},
                device_id_type=MESH,
            ).start()
            return carry

        lax.fori_loop(0, FREQ_DEVICES - 1, send, 0)

    adj_at = lambda k, f: adj.at[k, f]
    got1_at = lambda k, f: got1.at[k, :, pl.ds(pl.multiple_of(16 * f, 16), 16), :]
    send2_at = lambda k, f: send2.at[k, :, pl.ds(pl.multiple_of(16 * f, 16), 16), :]
    got2_at = lambda k, f: got2.at[k, f]

    own1, own2 = [], []
    for k in range(2):
        loads[2 * k].wait()
        loads[2 * k + 1].wait()
        operands(k)
        both = mm(vh[...], gh[k]) + mm(vh[...], gl[k]) + mm(vl[...], gh[k])
        for c in range(4):
            quarter = both[:, c * 128 : c * 128 + 128].reshape(FREQ_DEVICES, JD, 128)
            adj[k, :, c % 2, c // 2 * JD : c // 2 * JD + JD, :] = quarter
        if k == 0:
            pl.semaphore_wait(barrier, FREQ_DEVICES - 1 + len(friends))
        exchange(k, adj_at, got1_at, send_sem1, recv_sem1)
        own1.append(pltpu.make_async_copy(adj_at(k, me), got1_at(k, me), self_sem.at[k]))
        own1[k].start()

    band = bands_ref[...]
    own_rate = jnp.zeros((JD, CD), F32)
    for b in range(BANDS):
        own_rate = own_rate + jnp.where(band == b, rates_ref[b], 0.0)
    rate[:, 0:CD] = own_rate

    def all_but_one(buffer, k, send_sem, recv_sem):
        return pltpu.make_async_remote_copy(
            src_ref=buffer,
            dst_ref=buffer,
            send_sem=send_sem.at[k],
            recv_sem=recv_sem.at[k],
            device_id={"core": 1 - core},
            device_id_type=MESH,
        )

    for k in range(2):
        own1[k].wait()
        all_but_one(got1.at[k, :, pl.ds(0, 47 * 16), :], k, send_sem1, recv_sem1).wait_recv()

    time = lax.broadcasted_iota(jnp.int32, (TP, CD), 0)
    lane = lax.broadcasted_iota(jnp.int32, (TP // 4, 128), 1)
    to_left = jnp.zeros((TP // 4, 128), F32)
    to_right = jnp.zeros((TP // 4, 128), F32)
    for j in range(JD):
        value = jnp.concatenate(
            [
                jnp.concatenate([got1[k, h, pl.ds(j, NF, stride=JD), :] for h in range(2)], axis=1)
                for k in range(2)
            ],
            axis=0,
        )
        high, low = split(value)
        main = mm(inv_ref[...], high)
        series = main[0:TP] + main[TP:] + mm(inv_ref[0:TP], low)
        series = jnp.where(time < cut_ref[JD * me + j], series, 0.0)
        ext[j, :, 0:CD] = series
        for g in range(4):
            rows = slice(g * 24, g * 24 + 24)
            at = 32 * g + 4 * j
            here = (lane >= at) & (lane < at + 4)
            head, tail = series[rows, 0:128], series[rows, 128:256]
            head = pltpu.roll(head, at, 1) if at else head
            tail = pltpu.roll(tail, (at + 4) % 128, 1) if (at + 4) % 128 else tail
            to_left = jnp.where(here, head, to_left)
            to_right = jnp.where(here, tail, to_right)
    pack[0, 0:24] = to_left
    pack[1, 0:24] = to_right
    pack[0, 24:32] = own_rate[:, 0:128]
    pack[1, 24:32] = own_rate[:, 128:256]

    edge = []
    for side, friend in ((0, left), (1, right)):
        edge.append(
            pltpu.make_async_remote_copy(
                src_ref=pack.at[side],
                dst_ref=halo.at[side],
                send_sem=hsend.at[side],
                recv_sem=hrecv.at[side],
                device_id=friend,
                device_id_type=MESH,
            )
        )
        edge[side].start()
    for copy in edge:
        copy.wait()

    after = jnp.where(cell < 15, 1.0, 0.0)
    before = jnp.where(cell > 0, 1.0, 0.0)
    from_right, from_left = halo[0, 0:24] * after, halo[1, 0:24] * before
    lane8 = lax.broadcasted_iota(jnp.int32, (JD, 128), 1)
    far = jnp.where(lane8 < 4, halo[0, 24:32] * after, 0.0)
    far = jnp.where(lane8 >= 124, halo[1, 24:32] * before, far)
    rate[:, CD:] = far
    lane24 = lax.broadcasted_iota(jnp.int32, (TP // 4, 128), 1)

    for j in range(JD):
        for g in range(4):
            at = 32 * g + 4 * j
            first = pltpu.roll(from_right, 128 - at, 1) if at else from_right
            last = pltpu.roll(from_left, (252 - at) % 128, 1) if (252 - at) % 128 else from_left
            tile = jnp.where(lane24 < 4, first, jnp.where(lane24 >= 124, last, 0.0))
            ext[j, g * 24 : g * 24 + 24, CD:] = tile

    def smooth(j, carry):
        field = ext[j]
        rates = rate[0:1, :]
        for _ in range(SWEEPS):
            field = field + rates * (
                pltpu.roll(field, 1, 1) - 2.0 * field + pltpu.roll(field, CD + 127, 1)
            )
        high, low = split(field[:, 0:CD])
        uh[j] = high
        ul[j] = low
        return carry

    lax.fori_loop(0, JD, smooth, 0)

    for k in range(2):
        for j in range(JD):
            main = mm(fwd_ref[k], uh[j])
            main = main[0:NF] + main[NF:] + mm(fwd_ref[k, 0:NF], ul[j])
            for h in range(2):
                send2[k, h, pl.ds(j, NF, stride=JD), :] = main[:, h * 128 : h * 128 + 128]
        exchange(k, send2_at, got2_at, send_sem2, recv_sem2)
        own2.append(pltpu.make_async_copy(send2_at(k, me), got2_at(k, me), self_sem.at[2 + k]))
        own2[k].start()

    def move(k, i, source, target, friend):
        return pltpu.make_async_remote_copy(
            src_ref=source,
            dst_ref=target,
            send_sem=rsend.at[k, i],
            recv_sem=rrecv.at[k, i],
            device_id=friend,
            device_id_type=MESH,
        )

    for k in range(2):
        own2[k].wait()
        all_but_one(got2.at[k, pl.ds(0, 47)], k, send_sem2, recv_sem2).wait_recv()
        quarters = [
            split(got2[k, :, c % 2, c // 2 * JD : c // 2 * JD + JD, :].reshape(NJ, 128))
            for c in range(4)
        ]
        ch = jnp.concatenate([high for high, _ in quarters], axis=1)
        cl = jnp.concatenate([low for _, low in quarters], axis=1)
        for h in range(2):
            rows = slice(h * NSP, h * NSP + NSP)
            res = mt(ch, gh[k, rows, :]) + mt(ch, gl[k, rows, :]) + mt(cl, gh[k, rows, :])
            for c in range(16):
                part[k, c % 2, h, c // 4, (c // 2) % 2] = res[c * OUT_COLS : (c + 1) * OUT_COLS]
        mine = part.at[k, core]
        s1 = move(k, 0, part.at[k, 1 - core], r1.at[k], sibling)
        s1.start()
        s1.wait()
        part[k, core] = part[k, core] + r1[k]
        s2 = [
            move(k, 1, mine.at[0, swap], r2a.at[k, 0, 0], {"x": swap}),
            move(k, 2, mine.at[0, flip_swap], r2a.at[k, 0, 1], {"x": swap}),
            move(k, 3, mine.at[1, flip], r2a.at[k, 1, 0], {"x": flip}),
            move(k, 4, mine.at[1, flip_swap], r2a.at[k, 1, 1], {"x": flip}),
        ]
        for copy in s2:
            copy.start()
        for copy in s2:
            copy.wait()
        part[k, core, 0, flip] = part[k, core, 0, flip] + r2a[k, 0, 1]
        part[k, core, 1, swap] = part[k, core, 1, swap] + r2a[k, 1, 1]
        s3 = [
            move(k, 5, mine.at[0, flip], r2b.at[k, 0], {"x": flip}),
            move(k, 6, mine.at[1, swap], r2b.at[k, 1], {"x": swap}),
        ]
        for copy in s3:
            copy.start()
        for copy in s3:
            copy.wait()
        for h in range(2):
            part[k, core, h, x] = part[k, core, h, x] + r2a[k, h, 0] + r2b[k, h]
        s4 = [move(k, 7 + h, mine.at[h, x, 1 - yhi], r3.at[k, h], over) for h in range(2)]
        for copy in s4:
            copy.start()
        for copy in s4:
            copy.wait()
        for h in range(2):
            total = part[k, core, h, x, yhi] + r3[k, h]
            out_ref[h, k] = total[:, 0:NS]

    for k in range(2):
        all_but_one(got1.at[k, :, pl.ds(0, 47 * 16), :], k, send_sem1, recv_sem1).wait_send()
        all_but_one(got2.at[k, pl.ds(0, 47)], k, send_sem2, recv_sem2).wait_send()


def on_device(columns, freq_blocks, causal_cutoffs, band_index, band_rates):
    inverse, forward = tables()
    vmem = pl.BlockSpec(memory_space=pltpu.VMEM)
    smem = pl.BlockSpec(memory_space=pltpu.SMEM)
    anywhere = pl.BlockSpec(memory_space=pl.ANY)
    dma = pltpu.SemaphoreType.DMA
    return pl.pallas_call(
        kernel,
        out_shape=jax.ShapeDtypeStruct((2, 2, OUT_COLS, NS), F32),
        in_specs=[smem, smem, anywhere, anywhere, vmem, vmem, vmem],
        out_specs=vmem,
        scratch_shapes=[
            pltpu.VMEM((2, 2, NJ, NS), F32),
            pltpu.VMEM((2, 2, NS, CD), F32),
            pltpu.VMEM((NJ, 2 * NSP), BF16),
            pltpu.VMEM((NJ, 2 * NSP), BF16),
            pltpu.VMEM((2, 2 * NSP, 2 * CD), BF16),
            pltpu.VMEM((2, 2 * NSP, 2 * CD), BF16),
            pltpu.VMEM((2, FREQ_DEVICES, 2, 2 * JD, 128), F32),
            pltpu.VMEM((2, 2, NF * JD, 128), F32),
            pltpu.VMEM((JD, TP, CD + 128), F32),
            pltpu.VMEM((JD, TP, CD), BF16),
            pltpu.VMEM((JD, TP, CD), BF16),
            pltpu.VMEM((JD, CD + 128), F32),
            pltpu.VMEM((2, 32, 128), F32),
            pltpu.VMEM((2, 32, 128), F32),
            pltpu.VMEM((2, 2, NF * JD, 128), F32),
            pltpu.VMEM((2, FREQ_DEVICES, 2, 2 * JD, 128), F32),
            pltpu.VMEM((2, CORES, 2, EX, YHI, OUT_COLS, NSP), F32),
            pltpu.VMEM((2, 2, EX, YHI, OUT_COLS, NSP), F32),
            pltpu.VMEM((2, 2, 2, YHI, OUT_COLS, NSP), F32),
            pltpu.VMEM((2, 2, YHI, OUT_COLS, NSP), F32),
            pltpu.VMEM((2, 2, OUT_COLS, NSP), F32),
            dma((4,)),
            dma((4,)),
            dma((2,)),
            dma((2,)),
            dma((2,)),
            dma((2,)),
            dma((2,)),
            dma((2,)),
            dma((2, 9)),
            dma((2, 9)),
        ],
        compiler_params=pltpu.CompilerParams(
            collective_id=0, has_side_effects=True, vmem_limit_bytes=60 * 1024 * 1024
        ),
        name="hessian",
    )(
        causal_cutoffs,
        band_rates,
        columns,
        freq_blocks,
        jnp.broadcast_to(band_index[None, :], (JD, CD)),
        jnp.asarray(inverse),
        jnp.asarray(forward),
    )


def solution(mesh):
    torus = Mesh(mesh.devices.reshape(YLO, ZED, EX, YHI, CORES), AXES)
    freq, cell = ("ylo", "z"), ("x", "yhi", "core")
    placed = (P(None, freq, None, None), P(None, freq, None, cell), P(), P(cell), P())
    return jax.shard_map(
        on_device,
        mesh=torus,
        in_specs=placed,
        out_specs=P(None, freq, cell, None),
        check_vma=False,
    )
```

```python
import math

import jax
import jax.numpy as jnp
import numpy as np
from jax import lax
from jax.experimental import pallas as pl
from jax.experimental.pallas import tpu as pltpu
from jax.sharding import Mesh
from jax.sharding import PartitionSpec as P

AXES = ("ylo", "z", "x", "yhi", "core")
YLO, ZED, EX, YHI, CORES = 4, 12, 4, 2, 2
FREQ_DEVICES = YLO * ZED
NF = 96
NT = 95
TP = 96
NS = 600
NSP = 640
NJ = 384
JD = 8
CD = 256
SWEEPS = 4
BANDS = 8
OUT_COLS = 24
MESH = pl.DeviceIdType.MESH
F32, BF16 = jnp.float32, jnp.bfloat16


def halves(table):
    high = table.astype(np.float32).astype(jnp.bfloat16)
    low = (table - high.astype(np.float64)).astype(jnp.bfloat16)
    return high, low


def tables():
    cycle = 2 * NT
    k = np.arange(NF)
    t = np.arange(NT)
    angle = 2.0 * math.pi * ((t[:, None] * k[None, :]) % cycle) / cycle
    weight = np.where((k == 0) | (k == NF - 1), 1.0, 2.0) / cycle
    inv = np.stack([weight * np.cos(angle), -weight * np.sin(angle)], axis=-1)
    inv = inv.reshape(NT, FREQ_DEVICES, 2, 2).transpose(0, 2, 1, 3).reshape(NT, 2 * NF)
    inv = np.concatenate([inv, np.zeros((TP - NT, 2 * NF))], axis=0)
    fwd = np.stack([np.cos(angle), -np.sin(angle)], axis=-1)
    fwd = fwd.reshape(NT, FREQ_DEVICES, 2, 2).transpose(2, 1, 3, 0).reshape(2, NF, NT)
    fwd = np.concatenate([fwd, np.zeros((2, NF, TP - NT))], axis=2)
    return (
        np.concatenate(halves(inv), axis=0),
        np.concatenate(halves(fwd), axis=1),
    )


def split(x):
    high = x.astype(BF16)
    return high, (x - high.astype(F32)).astype(BF16)


def mm(a, b):
    return lax.dot_general(a, b, (((1,), (0,)), ((), ())), preferred_element_type=F32)


def mt(a, b):
    return lax.dot_general(a, b, (((1,), (1,)), ((), ())), preferred_element_type=F32)


def kernel(
    cut_ref, rates_ref, cols_ref, blocks_ref, bands_ref, inv_ref, fwd_ref, out_ref,
    cols, blocks, vh, vl, gh, gl, adj, got1, ext, uh, ul, rate, pack, halo, send2, got2,
    part, r1, r2, r3,
    load_sem, self_sem, ssem1, rsem1, ssem2, rsem2, hsend, hrecv, rsend, rrecv,
):
    y, z = lax.axis_index("ylo"), lax.axis_index("z")
    x, yhi, core = lax.axis_index("x"), lax.axis_index("yhi"), lax.axis_index("core")
    me = y * ZED + z
    cell = (x * YHI + yhi) * CORES + core

    loads = []
    for k in range(2):
        loads.append(pltpu.make_async_copy(cols_ref.at[:, k], cols.at[k], load_sem.at[2 * k]))
        loads.append(pltpu.make_async_copy(blocks_ref.at[:, k], blocks.at[k], load_sem.at[2 * k + 1]))
    for copy in loads:
        copy.start()

    rows_of_peers = [lax.rem(y + 3 - turn, YLO) for turn in range(4)]

    def for_peers(act):
        def some(step, count):
            half = 5 - lax.div(step - 1, 2)
            dz = jnp.where(lax.rem(step, 2) == 1, half, 12 - half)
            dz = jnp.where(step == 0, 6, jnp.where(step == 11, 0, dz))
            pz = lax.rem(z + dz, ZED)
            for py in rows_of_peers[:count]:
                act(py, pz)

        def body(step, carry):
            some(step, 4)
            return carry

        lax.fori_loop(0, 11, body, 0)
        some(jnp.int32(11), 3)

    def cell_peer(c):
        c = lax.rem(c + 16, 16)
        return {"x": lax.div(c, 4), "yhi": lax.rem(lax.div(c, 2), 2), "core": lax.rem(c, 2)}

    left, right = cell_peer(cell - 1), cell_peer(cell + 1)
    sibling, over = {"core": 1 - core}, {"yhi": 1 - yhi}
    across = [{"x": lax.rem(x + d, EX)} for d in (1, 2, 3)]

    barrier = pltpu.get_barrier_semaphore()

    def greet(py, pz):
        pl.semaphore_signal(barrier, inc=1, device_id={"ylo": py, "z": pz}, device_id_type=MESH)

    for_peers(greet)
    friends = [left, right, sibling, over, *across]
    for friend in friends:
        pl.semaphore_signal(barrier, inc=1, device_id=friend, device_id_type=MESH)

    def remote(source, target, send_sem, recv_sem, friend):
        return pltpu.make_async_remote_copy(
            src_ref=source,
            dst_ref=target,
            send_sem=send_sem,
            recv_sem=recv_sem,
            device_id=friend,
            device_id_type=MESH,
        )

    def rows8(f):
        return pl.ds(pl.multiple_of(8 * f, 8), 8)

    def exchange(source, target, send_sem, recv_sem):
        def send(py, pz):
            friend = {"ylo": py, "z": pz}
            remote(source(py * ZED + pz), target(me), send_sem, recv_sem, friend).start()

        for_peers(send)

    def arrived(buffer, sem):
        remote(buffer, buffer, sem, sem, sibling).wait_recv()

    def left_here(buffer, sem):
        remote(buffer, buffer, sem, sem, sibling).wait_send()

    top8 = lax.broadcasted_iota(jnp.int32, (1, JD, 128), 1) < 4

    def operands(k):
        for p in range(2):
            value = jnp.concatenate([cols[k, p], jnp.zeros((NSP - NS, NJ), F32)], axis=0)
            high, low = split(value.T)
            vh[:, p * NSP : p * NSP + NSP] = high
            vl[:, p * NSP : p * NSP + NSP] = low
        for p in range(2):
            value = jnp.concatenate([blocks[k, p], jnp.zeros((NSP - NS, CD), F32)], axis=0)
            high, low = split(value)
            for into, half in ((gh, high), (gl, low)):
                if p == 0:
                    into[k, 0:NSP, 0:CD] = half
                    into[k, NSP:, CD:] = half
                else:
                    into[k, 0:NSP, CD:] = -half
                    into[k, NSP:, 0:CD] = half

    own1, own2 = [], []
    for k in range(2):
        loads[2 * k].wait()
        loads[2 * k + 1].wait()
        operands(k)
        both = mm(vh[...], gh[k]) + mm(vh[...], gl[k]) + mm(vl[...], gh[k])
        for h in range(2):
            real = both[:, h * 128 : h * 128 + 128].reshape(FREQ_DEVICES, JD, 128)
            imag = both[:, CD + h * 128 : CD + h * 128 + 128].reshape(FREQ_DEVICES, JD, 128)
            adj[0, :, k, h] = jnp.where(top8, real, pltpu.roll(imag, 4, 1))
            adj[1, :, k, h] = jnp.where(top8, pltpu.roll(real, 4, 1), imag)
        if k == 0:
            pl.semaphore_wait(barrier, FREQ_DEVICES - 1 + len(friends))
        exchange(
            lambda f: adj.at[0, f, k], lambda f: got1.at[0, k, :, rows8(f), :], ssem1.at[0], rsem1.at[0]
        )
    exchange(lambda f: adj.at[1, f], lambda f: got1.at[1, :, :, rows8(f), :], ssem1.at[1], rsem1.at[1])
    for a in range(2):
        own1.append(
            pltpu.make_async_copy(adj.at[a, me], got1.at[a, :, :, rows8(me), :], self_sem.at[a])
        )
        own1[a].start()

    band = jnp.broadcast_to(bands_ref[...], (JD, CD))
    own_rate = jnp.zeros((JD, CD), F32)
    for b in range(BANDS):
        own_rate = own_rate + jnp.where(band == b, rates_ref[b], 0.0)
    rate[:, 0:CD] = own_rate

    time = lax.broadcasted_iota(jnp.int32, (TP, CD), 0)
    lane = lax.broadcasted_iota(jnp.int32, (TP // 4, 128), 1)
    lane8 = lax.broadcasted_iota(jnp.int32, (JD, 128), 1)
    after = jnp.where(cell < 15, 1.0, 0.0)
    before = jnp.where(cell > 0, 1.0, 0.0)

    def middle(a):
        own1[a].wait()
        arrived(got1.at[a, :, :, pl.ds(0, 47 * 8), :], rsem1.at[a])
        to_left = jnp.zeros((TP // 4, 128), F32)
        to_right = jnp.zeros((TP // 4, 128), F32)
        for j in range(4):
            value = jnp.concatenate(
                [
                    jnp.concatenate(
                        [got1[a, k, h, pl.ds(j, NF, stride=4), :] for h in range(2)], axis=1
                    )
                    for k in range(2)
                ],
                axis=0,
            )
            high, low = split(value)
            main = mm(inv_ref[...], high)
            series = main[0:TP] + main[TP:] + mm(inv_ref[0:TP], low)
            series = jnp.where(time < cut_ref[JD * me + 4 * a + j], series, 0.0)
            ext[a, j, :, 0:CD] = series
            for g in range(4):
                rows = slice(g * 24, g * 24 + 24)
                at = 32 * g + 4 * j
                here = (lane >= at) & (lane < at + 4)
                head, tail = series[rows, 0:128], series[rows, 128:256]
                head = pltpu.roll(head, at, 1) if at else head
                tail = pltpu.roll(tail, at + 4, 1)
                to_left = jnp.where(here, head, to_left)
                to_right = jnp.where(here, tail, to_right)
        pack[a, 0, 0:24] = to_left
        pack[a, 1, 0:24] = to_right
        pack[a, 0, 24:32] = rate[:, 0:128]
        pack[a, 1, 24:32] = rate[:, 128:256]
        edge = [
            remote(pack.at[a, side], halo.at[a, side], hsend.at[a, side], hrecv.at[a, side], friend)
            for side, friend in ((0, left), (1, right))
        ]
        for copy in edge:
            copy.start()
        for copy in edge:
            copy.wait()

        from_right, from_left = halo[a, 0, 0:24] * after, halo[a, 1, 0:24] * before
        far = jnp.where(lane8 < 4, halo[a, 0, 24:32] * after, 0.0)
        far = jnp.where(lane8 >= 124, halo[a, 1, 24:32] * before, far)
        rate[:, CD:] = far
        for j in range(4):
            for g in range(4):
                at = 32 * g + 4 * j
                first = pltpu.roll(from_right, 128 - at, 1) if at else from_right
                last = pltpu.roll(from_left, (252 - at) % 128, 1)
                tile = jnp.where(lane < 4, first, jnp.where(lane >= 124, last, 0.0))
                ext[a, j, g * 24 : g * 24 + 24, CD:] = tile

        def smooth(j, carry):
            field = ext[a, j]
            rates = rate[0:1, :]
            for _ in range(SWEEPS):
                field = field + rates * (
                    pltpu.roll(field, 1, 1) - 2.0 * field + pltpu.roll(field, CD + 127, 1)
                )
            high, low = split(field[:, 0:CD])
            uh[4 * a + j] = high
            ul[4 * a + j] = low
            return carry

        lax.fori_loop(0, 4, smooth, 0)

        for k in range(2):
            for j in range(4):
                main = mm(fwd_ref[k], uh[4 * a + j])
                main = main[0:NF] + main[NF:] + mm(fwd_ref[k, 0:NF], ul[4 * a + j])
                for h in range(2):
                    send2[a, k, h, pl.ds(j, NF, stride=4), :] = main[:, h * 128 : h * 128 + 128]
            if a == 1:
                exchange(
                    lambda f: send2.at[1, k, :, rows8(f), :],
                    lambda f: got2.at[1, f, k],
                    ssem2.at[1 + k],
                    rsem2.at[1 + k],
                )
        if a == 0:
            exchange(
                lambda f: send2.at[0, :, :, rows8(f), :], lambda f: got2.at[0, f], ssem2.at[0], rsem2.at[0]
            )
        own2.append(
            pltpu.make_async_copy(send2.at[a, :, :, rows8(me), :], got2.at[a, me], self_sem.at[2 + a])
        )
        own2[a].start()

    class Unit:
        def __init__(self, index, a, k, low, high):
            self.a, self.k, self.u = a, k, 2 * a + k
            self.low, self.high = low, high
            lanes = pl.ds(low, high - low)
            whole, u = part.at[self.u], self.u
            self.first = [
                remote(
                    whole.at[1 - core, :, :, :, lanes], r1.at[u, :, :, :, lanes],
                    rsend.at[index, 0], rrecv.at[index, 0], sibling,
                )
            ]
            self.second = [
                remote(
                    whole.at[core, lax.rem(x + d + 1, EX), :, :, lanes], r2.at[u, d, :, :, lanes],
                    rsend.at[index, 1 + d], rrecv.at[index, 1 + d], across[d],
                )
                for d in (1, 0, 2)
            ]
            self.third = [
                remote(
                    whole.at[core, x, 1 - yhi, :, lanes], r3.at[u, :, lanes],
                    rsend.at[index, 4], rrecv.at[index, 4], over,
                )
            ]

        def multiply(self):
            a, k = self.a, self.k
            low, high = self.low, self.high
            quarters = [split(got2[a, :, k, h].reshape(NJ, 128)) for h in range(2)]
            ch = jnp.concatenate([q[0] for q in quarters], axis=1)
            cl = jnp.concatenate([q[1] for q in quarters], axis=1)

            def product(start):
                rows = slice(start + low, start + high)
                gr, gs = gh[k, rows, 0:CD], gl[k, rows, 0:CD]
                return mt(ch, gr) + mt(ch, gs) + mt(cl, gr)

            width = high - low
            plain = product(0).reshape(FREQ_DEVICES, JD, width)
            cross = pltpu.roll(product(NSP).reshape(FREQ_DEVICES, JD, width), 4, 1)
            top = lax.broadcasted_iota(jnp.int32, (1, JD, width), 1) < 4
            total = (plain + jnp.where(top, -cross, cross)).reshape(NJ, width)
            for c in range(16):
                part[self.u, c % 2, c // 4, (c // 2) % 2, :, low:high] = total[
                    c * OUT_COLS : (c + 1) * OUT_COLS
                ]
            for copy in self.first:
                copy.start()

        def after_first(self):
            lanes, u = slice(self.low, self.high), self.u
            for copy in self.first:
                copy.wait()
            part[u, core, :, :, :, lanes] = part[u, core, :, :, :, lanes] + r1[u, :, :, :, lanes]
            for copy in self.second:
                copy.start()

        def after_second(self):
            lanes, u = slice(self.low, self.high), self.u
            for copy in self.second:
                copy.wait()
            total = part[u, core, x, :, :, lanes]
            for d in range(3):
                total = total + r2[u, d, :, :, lanes]
            part[u, core, x, :, :, lanes] = total
            for copy in self.third:
                copy.start()

        def after_third(self):
            lanes, u = slice(self.low, self.high), self.u
            for copy in self.third:
                copy.wait()
            r3[u, :, lanes] = part[u, core, x, yhi, :, lanes] + r3[u, :, lanes]

    middle(0)
    middle(1)

    own2[0].wait()
    arrived(got2.at[0, pl.ds(0, 47)], rsem2.at[0])
    ua, ub, uc = Unit(0, 0, 0, 0, NSP), Unit(1, 0, 1, 0, NSP), Unit(2, 1, 0, 0, NSP)
    ud, ue = Unit(3, 1, 1, 0, 384), Unit(4, 1, 1, 384, NSP)
    ua.multiply()
    ub.multiply()
    ua.after_first()
    ub.after_first()
    ua.after_second()
    own2[1].wait()
    arrived(got2.at[1, pl.ds(0, 47), 0], rsem2.at[1])
    uc.multiply()
    ub.after_second()
    uc.after_first()
    ua.after_third()
    uc.after_second()
    arrived(got2.at[1, pl.ds(0, 47), 1], rsem2.at[2])
    ud.multiply()
    ue.multiply()
    ub.after_third()
    ud.after_first()
    ue.after_first()
    ud.after_second()
    ue.after_second()
    uc.after_third()
    ud.after_third()
    ue.after_third()

    top = lax.broadcasted_iota(jnp.int32, (JD, NS), 0) < 4
    for k in range(2):
        for t in range(3):
            rows = slice(8 * t, 8 * t + 8)
            first, last = r3[k, rows, 0:NS], r3[2 + k, rows, 0:NS]
            out_ref[0, k, rows] = jnp.where(top, first, pltpu.roll(last, 4, 0))
            out_ref[1, k, rows] = jnp.where(top, pltpu.roll(first, 4, 0), last)

    for a in range(2):
        left_here(got1.at[a, :, :, pl.ds(0, 47 * 8), :], ssem1.at[a])
    left_here(got2.at[0, pl.ds(0, 47)], ssem2.at[0])
    for k in range(2):
        left_here(got2.at[1, pl.ds(0, 47), k], ssem2.at[1 + k])


def on_device(columns, freq_blocks, causal_cutoffs, band_index, band_rates):
    inverse, forward = tables()
    vmem = pl.BlockSpec(memory_space=pltpu.VMEM)
    smem = pl.BlockSpec(memory_space=pltpu.SMEM)
    anywhere = pl.BlockSpec(memory_space=pl.ANY)
    dma = pltpu.SemaphoreType.DMA
    return pl.pallas_call(
        kernel,
        out_shape=jax.ShapeDtypeStruct((2, 2, OUT_COLS, NS), F32),
        in_specs=[smem, smem, anywhere, anywhere, vmem, vmem, vmem],
        out_specs=vmem,
        scratch_shapes=[
            pltpu.VMEM((2, 2, NS, NJ), F32),
            pltpu.VMEM((2, 2, NS, CD), F32),
            pltpu.VMEM((NJ, 2 * NSP), BF16),
            pltpu.VMEM((NJ, 2 * NSP), BF16),
            pltpu.VMEM((2, 2 * NSP, 2 * CD), BF16),
            pltpu.VMEM((2, 2 * NSP, 2 * CD), BF16),
            pltpu.VMEM((2, FREQ_DEVICES, 2, 2, JD, 128), F32),
            pltpu.VMEM((2, 2, 2, NF * 4, 128), F32),
            pltpu.VMEM((2, 4, TP, CD + 128), F32),
            pltpu.VMEM((JD, TP, CD), BF16),
            pltpu.VMEM((JD, TP, CD), BF16),
            pltpu.VMEM((JD, CD + 128), F32),
            pltpu.VMEM((2, 2, 32, 128), F32),
            pltpu.VMEM((2, 2, 32, 128), F32),
            pltpu.VMEM((2, 2, 2, NF * 4, 128), F32),
            pltpu.VMEM((2, FREQ_DEVICES, 2, 2, JD, 128), F32),
            pltpu.VMEM((4, CORES, EX, YHI, OUT_COLS, NSP), F32),
            pltpu.VMEM((4, EX, YHI, OUT_COLS, NSP), F32),
            pltpu.VMEM((4, 3, YHI, OUT_COLS, NSP), F32),
            pltpu.VMEM((4, OUT_COLS, NSP), F32),
            dma((4,)),
            dma((4,)),
            dma((2,)),
            dma((2,)),
            dma((3,)),
            dma((3,)),
            dma((2, 2)),
            dma((2, 2)),
            dma((5, 5)),
            dma((5, 5)),
        ],
        compiler_params=pltpu.CompilerParams(
            collective_id=0, has_side_effects=True, vmem_limit_bytes=60 * 1024 * 1024
        ),
        name="hessian",
    )(
        causal_cutoffs,
        band_rates,
        jnp.swapaxes(columns, 2, 3),
        freq_blocks,
        band_index.reshape(1, CD),
        jnp.asarray(inverse),
        jnp.asarray(forward),
    )


def solution(mesh):
    torus = Mesh(mesh.devices.reshape(YLO, ZED, EX, YHI, CORES), AXES)
    freq, cell = ("ylo", "z"), ("x", "yhi", "core")
    placed = (P(None, freq, None, None), P(None, freq, None, cell), P(), P(cell), P())
    return jax.shard_map(
        on_device,
        mesh=torus,
        in_specs=placed,
        out_specs=P(None, freq, cell, None),
        check_vma=False,
    )
```

```python
import math

import jax
import jax.numpy as jnp
import numpy as np
from jax import lax
from jax.experimental import pallas as pl
from jax.experimental.pallas import tpu as pltpu
from jax.sharding import Mesh
from jax.sharding import PartitionSpec as P

AXES = ("ylo", "z", "x", "yhi", "core")
YLO, ZED, EX, YHI, CORES = 4, 12, 4, 2, 2
FREQ_DEVICES = YLO * ZED
NF = 96
NT = 95
TP = 96
NS = 600
NSP = 640
NJ = 384
JD = 8
CD = 256
SWEEPS = 4
BANDS = 8
OUT_COLS = 24
MESH = pl.DeviceIdType.MESH
F32, BF16 = jnp.float32, jnp.bfloat16


def halves(table):
    high = table.astype(np.float32).astype(jnp.bfloat16)
    low = (table - high.astype(np.float64)).astype(jnp.bfloat16)
    return high, low


def tables():
    cycle = 2 * NT
    k = np.arange(NF)
    t = np.arange(NT)
    angle = 2.0 * math.pi * ((t[:, None] * k[None, :]) % cycle) / cycle
    weight = np.where((k == 0) | (k == NF - 1), 1.0, 2.0) / cycle
    inv = np.stack([weight * np.cos(angle), -weight * np.sin(angle)], axis=-1)
    inv = inv.reshape(NT, FREQ_DEVICES, 2, 2).transpose(0, 2, 1, 3).reshape(NT, 2 * NF)
    inv = np.concatenate([inv, np.zeros((TP - NT, 2 * NF))], axis=0)
    fwd = np.stack([np.cos(angle), -np.sin(angle)], axis=-1)
    fwd = fwd.reshape(NT, FREQ_DEVICES, 2, 2).transpose(2, 1, 3, 0).reshape(2, NF, NT)
    fwd = np.concatenate([fwd, np.zeros((2, NF, TP - NT))], axis=2)
    return (
        np.concatenate(halves(inv), axis=0),
        np.concatenate(halves(fwd), axis=1),
    )


def split(x):
    high = x.astype(BF16)
    return high, (x - high.astype(F32)).astype(BF16)


def mm(a, b):
    return lax.dot_general(a, b, (((1,), (0,)), ((), ())), preferred_element_type=F32)


def mt(a, b):
    return lax.dot_general(a, b, (((1,), (1,)), ((), ())), preferred_element_type=F32)


def kernel(
    cut_ref, rates_ref, cols_ref, blocks_ref, bands_ref, inv_ref, fwd_ref, out_ref,
    cols, blocks, vh, vl, gh, gl, adj, got1, ext, uh, ul, rate, pack, halo, send2, got2,
    part, r1, r2, r3,
    load_sem, self_sem, ssem1, rsem1, ssem2, rsem2, hsend, hrecv, rsend, rrecv,
):
    y, z = lax.axis_index("ylo"), lax.axis_index("z")
    x, yhi, core = lax.axis_index("x"), lax.axis_index("yhi"), lax.axis_index("core")
    me = y * ZED + z
    cell = (x * YHI + yhi) * CORES + core

    loads = []
    for k in range(2):
        loads.append(pltpu.make_async_copy(cols_ref.at[:, k], cols.at[k], load_sem.at[2 * k]))
        loads.append(pltpu.make_async_copy(blocks_ref.at[:, k], blocks.at[k], load_sem.at[2 * k + 1]))
    for copy in loads[0:2]:
        copy.start()

    rows_of_peers = [lax.rem(y + 3 - turn, YLO) for turn in range(4)]

    def for_peers(act):
        def some(step, count):
            half = 5 - lax.div(step - 1, 2)
            dz = jnp.where(lax.rem(step, 2) == 1, half, 12 - half)
            dz = jnp.where(step == 0, 6, jnp.where(step == 11, 0, dz))
            pz = lax.rem(z + dz, ZED)
            for py in rows_of_peers[:count]:
                act(py, pz)

        def body(step, carry):
            some(step, 4)
            return carry

        lax.fori_loop(0, 11, body, 0)
        some(jnp.int32(11), 3)

    def cell_peer(c):
        c = lax.rem(c + 16, 16)
        return {"x": lax.div(c, 4), "yhi": lax.rem(lax.div(c, 2), 2), "core": lax.rem(c, 2)}

    left, right = cell_peer(cell - 1), cell_peer(cell + 1)
    sibling, over = {"core": 1 - core}, {"yhi": 1 - yhi}
    across = [{"x": lax.rem(x + d, EX)} for d in (1, 2, 3)]

    barrier = pltpu.get_barrier_semaphore()

    def greet(py, pz):
        pl.semaphore_signal(barrier, inc=1, device_id={"ylo": py, "z": pz}, device_id_type=MESH)

    for_peers(greet)
    friends = [left, right, sibling, over, *across]
    for friend in friends:
        pl.semaphore_signal(barrier, inc=1, device_id=friend, device_id_type=MESH)

    def remote(source, target, send_sem, recv_sem, friend):
        return pltpu.make_async_remote_copy(
            src_ref=source,
            dst_ref=target,
            send_sem=send_sem,
            recv_sem=recv_sem,
            device_id=friend,
            device_id_type=MESH,
        )

    def rows8(f):
        return pl.ds(pl.multiple_of(8 * f, 8), 8)

    def exchange(source, target, send_sem, recv_sem):
        def send(py, pz):
            friend = {"ylo": py, "z": pz}
            remote(source(py * ZED + pz), target(me), send_sem, recv_sem, friend).start()

        for_peers(send)

    def arrived(buffer, sem):
        remote(buffer, buffer, sem, sem, sibling).wait_recv()

    def left_here(buffer, sem):
        remote(buffer, buffer, sem, sem, sibling).wait_send()

    top8 = lax.broadcasted_iota(jnp.int32, (1, JD, 128), 1) < 4

    def operands(k):
        for p in range(2):
            value = jnp.concatenate([cols[k, p], jnp.zeros((NSP - NS, NJ), F32)], axis=0)
            high, low = split(value.T)
            vh[:, p * NSP : p * NSP + NSP] = high
            vl[:, p * NSP : p * NSP + NSP] = low
        for p in range(2):
            value = jnp.concatenate([blocks[k, p], jnp.zeros((NSP - NS, CD), F32)], axis=0)
            high, low = split(value)
            for into, half in ((gh, high), (gl, low)):
                if p == 0:
                    into[k, 0:NSP, 0:CD] = half
                    into[k, NSP:, CD:] = half
                else:
                    into[k, 0:NSP, CD:] = -half
                    into[k, NSP:, 0:CD] = half

    own1, own2 = [], []
    for k in range(2):
        loads[2 * k].wait()
        loads[2 * k + 1].wait()
        if k == 0:
            for copy in loads[2:4]:
                copy.start()
        operands(k)
        both = mm(vh[...], gh[k]) + mm(vh[...], gl[k]) + mm(vl[...], gh[k])
        for h in range(2):
            real = both[:, h * 128 : h * 128 + 128].reshape(FREQ_DEVICES, JD, 128)
            imag = both[:, CD + h * 128 : CD + h * 128 + 128].reshape(FREQ_DEVICES, JD, 128)
            adj[0, :, k, h] = jnp.where(top8, real, pltpu.roll(imag, 4, 1))
            adj[1, :, k, h] = jnp.where(top8, pltpu.roll(real, 4, 1), imag)
        if k == 0:
            pl.semaphore_wait(barrier, FREQ_DEVICES - 1 + len(friends))
        exchange(
            lambda f: adj.at[0, f, k], lambda f: got1.at[0, k, :, rows8(f), :], ssem1.at[0], rsem1.at[0]
        )
    exchange(lambda f: adj.at[1, f], lambda f: got1.at[1, :, :, rows8(f), :], ssem1.at[1], rsem1.at[1])
    for a in range(2):
        own1.append(
            pltpu.make_async_copy(adj.at[a, me], got1.at[a, :, :, rows8(me), :], self_sem.at[a])
        )
        own1[a].start()

    band = jnp.broadcast_to(bands_ref[...], (JD, CD))
    own_rate = jnp.zeros((JD, CD), F32)
    for b in range(BANDS):
        own_rate = own_rate + jnp.where(band == b, rates_ref[b], 0.0)
    rate[:, 0:CD] = own_rate

    time = lax.broadcasted_iota(jnp.int32, (TP, CD), 0)
    lane = lax.broadcasted_iota(jnp.int32, (TP // 4, 128), 1)
    lane8 = lax.broadcasted_iota(jnp.int32, (JD, 128), 1)
    after = jnp.where(cell < 15, 1.0, 0.0)
    before = jnp.where(cell > 0, 1.0, 0.0)

    def middle(a):
        own1[a].wait()
        arrived(got1.at[a, :, :, pl.ds(0, 47 * 8), :], rsem1.at[a])
        to_left = jnp.zeros((TP // 4, 128), F32)
        to_right = jnp.zeros((TP // 4, 128), F32)
        for j in range(4):
            value = jnp.concatenate(
                [
                    jnp.concatenate(
                        [got1[a, k, h, pl.ds(j, NF, stride=4), :] for h in range(2)], axis=1
                    )
                    for k in range(2)
                ],
                axis=0,
            )
            high, low = split(value)
            main = mm(inv_ref[...], high)
            series = main[0:TP] + main[TP:] + mm(inv_ref[0:TP], low)
            series = jnp.where(time < cut_ref[JD * me + 4 * a + j], series, 0.0)
            ext[a, j, :, 0:CD] = series
            for g in range(4):
                rows = slice(g * 24, g * 24 + 24)
                at = 32 * g + 4 * j
                here = (lane >= at) & (lane < at + 4)
                head, tail = series[rows, 0:128], series[rows, 128:256]
                head = pltpu.roll(head, at, 1) if at else head
                tail = pltpu.roll(tail, at + 4, 1)
                to_left = jnp.where(here, head, to_left)
                to_right = jnp.where(here, tail, to_right)
        pack[a, 0, 0:24] = to_left
        pack[a, 1, 0:24] = to_right
        pack[a, 0, 24:32] = rate[:, 0:128]
        pack[a, 1, 24:32] = rate[:, 128:256]
        edge = [
            remote(pack.at[a, side], halo.at[a, side], hsend.at[a, side], hrecv.at[a, side], friend)
            for side, friend in ((0, left), (1, right))
        ]
        for copy in edge:
            copy.start()
        for copy in edge:
            copy.wait()

        from_right, from_left = halo[a, 0, 0:24] * after, halo[a, 1, 0:24] * before
        far = jnp.where(lane8 < 4, halo[a, 0, 24:32] * after, 0.0)
        far = jnp.where(lane8 >= 124, halo[a, 1, 24:32] * before, far)
        rate[:, CD:] = far
        for j in range(4):
            for g in range(4):
                at = 32 * g + 4 * j
                first = pltpu.roll(from_right, 128 - at, 1) if at else from_right
                last = pltpu.roll(from_left, (252 - at) % 128, 1)
                tile = jnp.where(lane < 4, first, jnp.where(lane >= 124, last, 0.0))
                ext[a, j, g * 24 : g * 24 + 24, CD:] = tile

        def smooth(j, carry):
            field = ext[a, j]
            rates = rate[0:1, :]
            for _ in range(SWEEPS):
                field = field + rates * (
                    pltpu.roll(field, 1, 1) - 2.0 * field + pltpu.roll(field, CD + 127, 1)
                )
            high, low = split(field[:, 0:CD])
            uh[4 * a + j] = high
            ul[4 * a + j] = low
            return carry

        lax.fori_loop(0, 4, smooth, 0)

        for k in range(2):
            for j in range(4):
                main = mm(fwd_ref[k], uh[4 * a + j])
                main = main[0:NF] + main[NF:] + mm(fwd_ref[k, 0:NF], ul[4 * a + j])
                for h in range(2):
                    send2[a, k, h, pl.ds(j, NF, stride=4), :] = main[:, h * 128 : h * 128 + 128]
            if a == 1:
                exchange(
                    lambda f: send2.at[1, k, :, rows8(f), :],
                    lambda f: got2.at[1, f, k],
                    ssem2.at[1 + k],
                    rsem2.at[1 + k],
                )
        if a == 0:
            exchange(
                lambda f: send2.at[0, :, :, rows8(f), :], lambda f: got2.at[0, f], ssem2.at[0], rsem2.at[0]
            )
        own2.append(
            pltpu.make_async_copy(send2.at[a, :, :, rows8(me), :], got2.at[a, me], self_sem.at[2 + a])
        )
        own2[a].start()

    class Unit:
        def __init__(self, index, a, k, low, high):
            self.a, self.k, self.u = a, k, 2 * a + k
            self.low, self.high = low, high
            lanes = pl.ds(low, high - low)
            whole, u = part.at[self.u], self.u
            self.first = [
                remote(
                    whole.at[1 - core, :, :, :, lanes], r1.at[u, :, :, :, lanes],
                    rsend.at[index, 0], rrecv.at[index, 0], sibling,
                )
            ]
            self.second = [
                remote(
                    whole.at[core, lax.rem(x + d + 1, EX), :, :, lanes], r2.at[u, d, :, :, lanes],
                    rsend.at[index, 1 + d], rrecv.at[index, 1 + d], across[d],
                )
                for d in (1, 0, 2)
            ]
            self.third = [
                remote(
                    whole.at[core, x, 1 - yhi, :, lanes], r3.at[u, :, lanes],
                    rsend.at[index, 4], rrecv.at[index, 4], over,
                )
            ]

        def multiply(self):
            a, k = self.a, self.k
            low, high = self.low, self.high
            quarters = [split(got2[a, :, k, h].reshape(NJ, 128)) for h in range(2)]
            ch = jnp.concatenate([q[0] for q in quarters], axis=1)
            cl = jnp.concatenate([q[1] for q in quarters], axis=1)

            def product(start):
                rows = slice(start + low, start + high)
                gr, gs = gh[k, rows, 0:CD], gl[k, rows, 0:CD]
                return mt(ch, gr) + mt(ch, gs) + mt(cl, gr)

            width = high - low
            plain = product(0).reshape(FREQ_DEVICES, JD, width)
            cross = pltpu.roll(product(NSP).reshape(FREQ_DEVICES, JD, width), 4, 1)
            top = lax.broadcasted_iota(jnp.int32, (1, JD, width), 1) < 4
            total = (plain + jnp.where(top, -cross, cross)).reshape(NJ, width)
            for c in range(16):
                part[self.u, c % 2, c // 4, (c // 2) % 2, :, low:high] = total[
                    c * OUT_COLS : (c + 1) * OUT_COLS
                ]
            for copy in self.first:
                copy.start()

        def after_first(self):
            lanes, u = slice(self.low, self.high), self.u
            for copy in self.first:
                copy.wait()
            part[u, core, :, :, :, lanes] = part[u, core, :, :, :, lanes] + r1[u, :, :, :, lanes]
            for copy in self.second:
                copy.start()

        def after_second(self):
            lanes, u = slice(self.low, self.high), self.u
            for copy in self.second:
                copy.wait()
            total = part[u, core, x, :, :, lanes]
            for d in range(3):
                total = total + r2[u, d, :, :, lanes]
            part[u, core, x, :, :, lanes] = total
            for copy in self.third:
                copy.start()

        def after_third(self):
            lanes, u = slice(self.low, self.high), self.u
            for copy in self.third:
                copy.wait()
            r3[u, :, lanes] = part[u, core, x, yhi, :, lanes] + r3[u, :, lanes]

    middle(0)
    middle(1)

    own2[0].wait()
    arrived(got2.at[0, pl.ds(0, 47)], rsem2.at[0])
    ua, ub, uc = Unit(0, 0, 0, 0, NSP), Unit(1, 0, 1, 0, NSP), Unit(2, 1, 0, 0, NSP)
    ud, ue, uf = Unit(3, 1, 1, 0, 256), Unit(4, 1, 1, 256, 512), Unit(5, 1, 1, 512, NSP)
    ua.multiply()
    ub.multiply()
    ua.after_first()
    ub.after_first()
    ua.after_second()
    own2[1].wait()
    arrived(got2.at[1, pl.ds(0, 47), 0], rsem2.at[1])
    uc.multiply()
    ub.after_second()
    uc.after_first()
    ua.after_third()
    arrived(got2.at[1, pl.ds(0, 47), 1], rsem2.at[2])
    ud.multiply()
    ue.multiply()
    ud.after_first()
    uf.multiply()
    ue.after_first()
    uf.after_first()
    uc.after_second()
    ub.after_third()
    ud.after_second()
    ue.after_second()
    uf.after_second()
    uc.after_third()
    ud.after_third()
    ue.after_third()
    uf.after_third()

    top = lax.broadcasted_iota(jnp.int32, (JD, NS), 0) < 4
    for k in range(2):
        for t in range(3):
            rows = slice(8 * t, 8 * t + 8)
            first, last = r3[k, rows, 0:NS], r3[2 + k, rows, 0:NS]
            out_ref[0, k, rows] = jnp.where(top, first, pltpu.roll(last, 4, 0))
            out_ref[1, k, rows] = jnp.where(top, pltpu.roll(first, 4, 0), last)

    for a in range(2):
        left_here(got1.at[a, :, :, pl.ds(0, 47 * 8), :], ssem1.at[a])
    left_here(got2.at[0, pl.ds(0, 47)], ssem2.at[0])
    for k in range(2):
        left_here(got2.at[1, pl.ds(0, 47), k], ssem2.at[1 + k])


def on_device(columns, freq_blocks, causal_cutoffs, band_index, band_rates):
    inverse, forward = tables()
    vmem = pl.BlockSpec(memory_space=pltpu.VMEM)
    smem = pl.BlockSpec(memory_space=pltpu.SMEM)
    anywhere = pl.BlockSpec(memory_space=pl.ANY)
    dma = pltpu.SemaphoreType.DMA
    return pl.pallas_call(
        kernel,
        out_shape=jax.ShapeDtypeStruct((2, 2, OUT_COLS, NS), F32),
        in_specs=[smem, smem, anywhere, anywhere, vmem, vmem, vmem],
        out_specs=vmem,
        scratch_shapes=[
            pltpu.VMEM((2, 2, NS, NJ), F32),
            pltpu.VMEM((2, 2, NS, CD), F32),
            pltpu.VMEM((NJ, 2 * NSP), BF16),
            pltpu.VMEM((NJ, 2 * NSP), BF16),
            pltpu.VMEM((2, 2 * NSP, 2 * CD), BF16),
            pltpu.VMEM((2, 2 * NSP, 2 * CD), BF16),
            pltpu.VMEM((2, FREQ_DEVICES, 2, 2, JD, 128), F32),
            pltpu.VMEM((2, 2, 2, NF * 4, 128), F32),
            pltpu.VMEM((2, 4, TP, CD + 128), F32),
            pltpu.VMEM((JD, TP, CD), BF16),
            pltpu.VMEM((JD, TP, CD), BF16),
            pltpu.VMEM((JD, CD + 128), F32),
            pltpu.VMEM((2, 2, 32, 128), F32),
            pltpu.VMEM((2, 2, 32, 128), F32),
            pltpu.VMEM((2, 2, 2, NF * 4, 128), F32),
            pltpu.VMEM((2, FREQ_DEVICES, 2, 2, JD, 128), F32),
            pltpu.VMEM((4, CORES, EX, YHI, OUT_COLS, NSP), F32),
            pltpu.VMEM((4, EX, YHI, OUT_COLS, NSP), F32),
            pltpu.VMEM((4, 3, YHI, OUT_COLS, NSP), F32),
            pltpu.VMEM((4, OUT_COLS, NSP), F32),
            dma((4,)),
            dma((4,)),
            dma((2,)),
            dma((2,)),
            dma((3,)),
            dma((3,)),
            dma((2, 2)),
            dma((2, 2)),
            dma((6, 5)),
            dma((6, 5)),
        ],
        compiler_params=pltpu.CompilerParams(
            collective_id=0, has_side_effects=True, vmem_limit_bytes=60 * 1024 * 1024
        ),
        name="hessian",
    )(
        causal_cutoffs,
        band_rates,
        jnp.swapaxes(columns, 2, 3),
        freq_blocks,
        band_index.reshape(1, CD),
        jnp.asarray(inverse),
        jnp.asarray(forward),
    )


def solution(mesh):
    torus = Mesh(mesh.devices.reshape(YLO, ZED, EX, YHI, CORES), AXES)
    freq, cell = ("ylo", "z"), ("x", "yhi", "core")
    placed = (P(None, freq, None, None), P(None, freq, None, cell), P(), P(cell), P())
    return jax.shard_map(
        on_device,
        mesh=torus,
        in_specs=placed,
        out_specs=P(None, freq, cell, None),
        check_vma=False,
    )
```
